32 devices in a mesh: gx: 4 (over z), gy: 4 (over y, x), gz: 2 (over core).
Axes of the slice: x: 2, y: 2, z: 4, core: 2. Of those that a mesh axis runs over, the one named last changes fastest.
Arguments:
- pair: bfloat16 [128, 128, 128], P('gx', ('gy', 'gz')), may hold values from -6 to 6
- pair_mask: int32 [128, 128], P('gx', ('gy', 'gz')), may hold values 0 or 1
- in_gain: float32 [128], replicated, may hold values from 0.1 to 1.9
- in_bias: float32 [128], replicated, may hold values from -3 to 3
- proj_weight: bfloat16 [128, 512], replicated, may hold values from -0.5 to 0.5
- gate_weight: bfloat16 [128, 128], replicated, may hold values from -0.5 to 0.5
- out_gain: float32 [128], replicated, may hold values from 0.1 to 1.9
- out_bias: float32 [128], replicated, may hold values from -3 to 3
- out_weight: bfloat16 [128, 128], replicated, may hold values from -0.5 to 0.5
Outputs:
- update: bfloat16 [128, 128, 128], P('gx', ('gy', 'gz'))
The draws below stay inside these ranges and needn't reach their ends.
All inputs are finite; a program needn't handle non-finite values. No bound on the sum of `pair_mask` on one device may be relied on, other than what follows from the above.
Results may differ from the reference program's by a relative error of at most 0.0071.
Values may be sent and summed in bfloat16 or wider, within the bound.
A program may use at most 64 MiB of HBM per device.

```python
import jax
import jax.numpy as jnp
from jax import lax

C = 128
CH = 128
N = 128


def with_ends(array, stream_key, smallest, high):
    spot = [jax.random.randint(jax.random.fold_in(stream_key, axis), (), 0, length) for axis, length in enumerate(array.shape)]
    widest = array.shape.index(max(array.shape))
    beside = spot[:widest] + [(spot[widest] + 1) % array.shape[widest]] + spot[widest + 1:]
    return array.at[tuple(spot)].set(smallest).at[tuple(beside)].set(high)


def block_levels(stream_key, shape, pieces, low, largest):
    loudness = 1.0
    for axis_at, parts in pieces:
        steps = jax.random.uniform(jax.random.fold_in(jax.random.fold_in(stream_key, 6), axis_at), (parts,), jnp.float32, low / len(pieces), largest / len(pieces))
        loudness = loudness * jnp.repeat(jnp.exp(steps), shape[axis_at] // parts).reshape((-1,) + (1,) * (len(shape) - 1 - axis_at))
    return loudness


def gaussian(key, shape, scale, reach, split=(), held_as=jnp.bfloat16):
    result = scale * jax.random.normal(key, shape, jnp.float32)
    if split:
        result = result * block_levels(key, shape, split, -0.22, 0.18)
    return jnp.clip(result, -reach, reach).astype(held_as)


def setup_inputs(seed: int = 0) -> dict:
    splits = jax.random.split(jax.random.key(seed), 10)
    pair = gaussian(splits[0], (N, N, C), 1.0, 6.0, ((0, 4), (1, 8)))
    pair_mask = with_ends((jax.random.randint(splits[1], (N, N), 0, 4) < 3).astype(jnp.int32), jax.random.fold_in(splits[1], 1), 0, 1)
    in_gain = jnp.clip(1.0 + 0.18 * jax.random.normal(splits[2], (C,), jnp.float32), 0.1, 1.9)
    in_bias = gaussian(splits[3], (C,), 0.5, 3.0, (), jnp.float32)
    proj_weight = gaussian(splits[4], (C, 4 * CH), C ** -0.5, 0.5)
    gate_weight = gaussian(splits[5], (C, C), C ** -0.5, 0.5)
    out_gain = jnp.clip(1.0 + 0.18 * jax.random.normal(splits[6], (CH,), jnp.float32), 0.1, 1.9)
    out_bias = gaussian(splits[7], (CH,), 0.5, 3.0, (), jnp.float32)
    out_weight = gaussian(splits[8], (CH, C), CH ** -0.5, 0.5)
    return dict(pair=pair, pair_mask=pair_mask, in_gain=in_gain, in_bias=in_bias, proj_weight=proj_weight, gate_weight=gate_weight, out_gain=out_gain, out_bias=out_bias, out_weight=out_weight)


def normalize(values, gain, bias):
    average = lax.optimization_barrier(jnp.mean(values, axis=-1, keepdims=True))
    centered = values - average
    variance = lax.optimization_barrier(jnp.mean(centered * centered, axis=-1, keepdims=True))
    return centered * lax.rsqrt(variance + 1e-05) * gain + bias

def reference(pair, pair_mask, in_gain, in_bias, proj_weight, gate_weight, out_gain, out_bias, out_weight):
    total = pair.shape[0]
    channels = pair.shape[2]
    hidden = proj_weight.shape[1] // 4
    normed = normalize(pair.astype(jnp.float32), in_gain, in_bias).astype(jnp.bfloat16)
    flat = normed.reshape(total * total, channels)
    projected = jnp.dot(flat, proj_weight, preferred_element_type=jnp.float32).reshape(total, total, 4 * hidden)
    mask_value = pair_mask.astype(jnp.float32)[:, :, None]
    left_side = (jax.nn.sigmoid(projected[:, :, :hidden]) * projected[:, :, hidden:2 * hidden] * mask_value).astype(jnp.bfloat16)
    right_side = (jax.nn.sigmoid(projected[:, :, 2 * hidden:3 * hidden]) * projected[:, :, 3 * hidden:] * mask_value).astype(jnp.bfloat16)
    triangle = jnp.einsum('ikc,jkc->ijc', left_side.astype(jnp.float32), right_side.astype(jnp.float32), precision=lax.Precision.HIGHEST)
    tri_normed = normalize(triangle, out_gain, out_bias).astype(jnp.bfloat16)
    gating = jax.nn.sigmoid(jnp.dot(flat, gate_weight, preferred_element_type=jnp.float32))
    mixed = jnp.dot(tri_normed.reshape(total * total, hidden), out_weight, preferred_element_type=jnp.float32)
    return (gating * mixed).reshape(total, total, channels).astype(jnp.bfloat16)
```

```python
import functools

import jax
import jax.numpy as jnp
from jax import lax
from jax.experimental import pallas as pl
from jax.experimental.pallas import tpu as pltpu
from jax.sharding import PartitionSpec as P

MESH = pl.DeviceIdType.MESH
LANES = 128
EPSILON = 1e-05
PIECES = 4


def normalize(values, gain, bias):
    average = jnp.mean(values, axis=-1, keepdims=True)
    centered = values - average
    variance = jnp.mean(centered * centered, axis=-1, keepdims=True)
    return centered * lax.rsqrt(variance + EPSILON) * gain + bias


def project(tile, mask_value, in_gain, in_bias, proj_weight):
    hidden = proj_weight.shape[1] // 4
    normed = normalize(tile.astype(jnp.float32), in_gain, in_bias).astype(jnp.bfloat16)
    projected = jnp.einsum("rwc,cd->rwd", normed, proj_weight, preferred_element_type=jnp.float32)
    left_side = (
        jax.nn.sigmoid(projected[:, :, :hidden]) * projected[:, :, hidden : 2 * hidden] * mask_value
    ).astype(jnp.bfloat16)
    right_side = (
        jax.nn.sigmoid(projected[:, :, 2 * hidden : 3 * hidden])
        * projected[:, :, 3 * hidden :]
        * mask_value
    ).astype(jnp.bfloat16)
    return (normed, left_side, right_side)


def with_collectives(
    pair, pair_mask, in_gain, in_bias, proj_weight, gate_weight, out_gain, out_bias, out_weight
):
    mask_value = pair_mask.astype(jnp.float32)[:, :, None]
    normed, left_side, own_right = project(pair, mask_value, in_gain, in_bias, proj_weight)
    left_slab, right_slab = (
        lax.all_gather(left_side, "gy", axis=1, tiled=True),
        lax.all_gather(own_right, "gy", axis=1, tiled=True),
    )
    every_row = lax.all_gather(own_right, "gx", axis=0, tiled=True)
    row_panel = lax.all_to_all(every_row, "gy", split_axis=0, concat_axis=1, tiled=True)
    summed = lax.psum_scatter(
        jnp.einsum("jkc,ikc->jic", row_panel, left_slab, preferred_element_type=jnp.float32),
        "gz",
        scatter_dimension=0,
        tiled=True,
    )
    triangle = jnp.transpose(summed, (1, 0, 2))
    tri_normed = normalize(triangle, out_gain, out_bias).astype(jnp.bfloat16)
    gating = jax.nn.sigmoid(
        jnp.einsum("rwc,cd->rwd", normed, gate_weight, preferred_element_type=jnp.float32)
    )
    mixed = jnp.einsum("rwh,hc->rwc", tri_normed, out_weight, preferred_element_type=jnp.float32)
    return (gating * mixed).astype(jnp.bfloat16)


def swap_groups(tiles, width):
    tiles = list(tiles)
    group = lax.broadcasted_iota(jnp.int32, tiles[0].shape, 1) // width
    bit = 1
    while bit < len(tiles):
        upper = (group // bit) % 2 == 1
        for a in range(len(tiles)):
            if (a // bit) % 2 == 0:
                low, high = tiles[a], tiles[a + bit]
                tiles[a] = jnp.where(upper, pltpu.roll(high, bit * width, 1), low)
                tiles[a + bit] = jnp.where(upper, high, pltpu.roll(low, LANES - bit * width, 1))
        bit *= 2
    return tiles


def kernel(
    nx,
    ny,
    nz,
    pair_ref,
    mask_ref,
    in_gain_ref,
    in_bias_ref,
    proj_ref,
    gate_ref,
    out_gain_ref,
    out_bias_ref,
    out_weight_ref,
    out_ref,
    right_out,
    left_out,
    tri_out,
    right_in,
    left_in,
    tri_in,
    right_all,
    left_all,
    spread,
    normed_ref,
    gating_ref,
    right_sems,
    left_sems,
    tri_sems,
    z_send,
    z_recv,
):
    rows, width, channels = pair_ref.shape
    hidden = proj_ref.shape[1] // 4
    plane = ny * nz
    block = hidden // plane
    tiles = rows * width // LANES
    per_tile = rows // tiles
    part = block // PIECES
    x, y, z = lax.axis_index("gx"), lax.axis_index("gy"), lax.axis_index("gz")
    me = y * nz + z

    def peer(t):
        d = lax.rem(me + t, plane)
        return d, (x, d // nz, lax.rem(d, nz))

    barrier = pltpu.get_barrier_semaphore()
    for t in range(1, plane):
        pl.semaphore_signal(barrier, inc=1, device_id=peer(t)[1], device_id_type=MESH)

    @pl.when(x > 0)
    def _():
        pl.semaphore_signal(barrier, inc=1, device_id=(x - 1, y, z), device_id_type=MESH)

    @pl.when(x < nx - 1)
    def _():
        pl.semaphore_signal(barrier, inc=1, device_id=(x + 1, y, z), device_id_type=MESH)

    normed = normalize(
        pair_ref[...].reshape(rows * width, channels).astype(jnp.float32),
        in_gain_ref[...],
        in_bias_ref[...],
    ).astype(jnp.bfloat16)
    normed_ref[...] = normed

    spot = lax.broadcasted_iota(jnp.int32, (width, rows * width), 1)
    choose = (spot % width == lax.broadcasted_iota(jnp.int32, spot.shape, 0)).astype(jnp.bfloat16)
    repeated = jnp.dot(
        mask_ref[...].astype(jnp.float32).astype(jnp.bfloat16), choose, preferred_element_type=jnp.float32
    )
    row_of = lax.broadcasted_iota(jnp.int32, repeated.shape, 1) // width
    own_row = row_of == lax.broadcasted_iota(jnp.int32, repeated.shape, 0)
    mask_row = jnp.sum(jnp.where(own_row, repeated, 0.0), axis=0, keepdims=True)

    def side(first, target):
        weight = proj_ref[:, first : first + 2 * hidden].T
        for q in range(tiles):
            lanes = slice(q * LANES, (q + 1) * LANES)
            projected = lax.dot_general(
                weight, normed_ref[lanes, :], (((1,), (1,)), ((), ())), preferred_element_type=jnp.float32
            )
            value = jax.nn.sigmoid(projected[:hidden]) * projected[hidden:] * mask_row[:, lanes]
            target[:, q] = value.astype(jnp.bfloat16).reshape(plane, block, LANES)

    def exchange(source, target, sems):
        copies = []
        for t in range(1, plane):
            d, device = peer(t)
            copies.append(
                pltpu.make_async_remote_copy(
                    src_ref=source.at[d],
                    dst_ref=target.at[me],
                    send_sem=sems.at[0, t],
                    recv_sem=sems.at[1, t],
                    device_id=device,
                    device_id_type=MESH,
                )
            )
            copies[-1].start()
        return copies

    def gather_sums(source, target):
        for q in range(tiles):
            swapped = swap_groups([source[a, q].astype(jnp.float32) for a in range(plane)], width)
            for a in range(per_tile):
                spread[pl.ds(q * per_tile + a, block, stride=rows), :] = swapped[a]
        target[...] = spread[...].astype(jnp.bfloat16).reshape(block, rows, LANES)

    side(2 * hidden, right_out)
    pl.semaphore_wait(
        barrier, plane - 1 + jnp.where(x > 0, 1, 0) + jnp.where(x < nx - 1, 1, 0)
    )
    right_copies = exchange(right_out, right_in, right_sems)
    right_in[me] = right_out[me]
    side(0, left_out)
    left_copies = exchange(left_out, left_in, left_sems)
    left_in[me] = left_out[me]
    gating_ref[...] = jax.nn.sigmoid(
        jnp.dot(normed_ref[...], gate_ref[...], preferred_element_type=jnp.float32)
    )

    for copy in right_copies:
        copy.wait_recv()
    gather_sums(right_in, right_all.at[x])

    def pass_on(way, t, piece):
        ahead = x + 1 if way == 0 else x - 1
        origin = x - t if way == 0 else x + t
        part_of = right_all.at[origin, pl.ds(piece * part, part)]
        return pltpu.make_async_remote_copy(
            src_ref=part_of,
            dst_ref=part_of,
            send_sem=z_send.at[way, t, piece],
            recv_sem=z_recv.at[way, t, piece],
            device_id=(ahead, y, z),
            device_id_type=MESH,
        )

    def has_ahead(way):
        return x < nx - 1 if way == 0 else x > 0

    def has_origin(way, t):
        return x >= t if way == 0 else x <= nx - 1 - t

    for piece in range(PIECES):
        for way in range(2):

            @pl.when(has_ahead(way))
            def _():
                pass_on(way, 0, piece).start()

    for copy in left_copies:
        copy.wait_recv()
    gather_sums(left_in, left_all)

    for t in range(1, nx):
        for piece in range(PIECES):
            for way in range(2):

                @pl.when(has_origin(way, t))
                def _():
                    pltpu.make_async_remote_copy(
                        src_ref=right_all.at[x, pl.ds(piece * part, part)],
                        dst_ref=right_all.at[x - t if way == 0 else x + t, pl.ds(piece * part, part)],
                        send_sem=z_send.at[way, t - 1, piece],
                        recv_sem=z_recv.at[way, t - 1, piece],
                        device_id=(x, y, z),
                        device_id_type=MESH,
                    ).wait_recv()
                    if t < nx - 1:

                        @pl.when(has_ahead(way))
                        def _():
                            pass_on(way, t, piece).start()

    for c in range(block):
        triangle = lax.dot_general(
            left_all[c],
            right_all[:, c].reshape(nx * rows, LANES),
            (((1,), (1,)), ((), ())),
            preferred_element_type=jnp.float32,
        )
        spread[pl.ds(c, rows, stride=block), :] = triangle
    for q in range(tiles):
        swapped = swap_groups(
            [spread[pl.ds((q * per_tile + a) * block, block), :] for a in range(per_tile)], width
        )
        for d in range(plane):
            tri_out[d, q] = swapped[d].astype(jnp.bfloat16)
    tri_copies = exchange(tri_out, tri_in, tri_sems)
    tri_in[me] = tri_out[me]
    for copy in tri_copies:
        copy.wait_recv()

    for q in range(tiles):
        lanes = slice(q * LANES, (q + 1) * LANES)
        sums = tri_in[:, q].reshape(hidden, LANES).astype(jnp.float32)
        centered = sums - jnp.mean(sums, axis=0, keepdims=True)
        variance = jnp.mean(centered * centered, axis=0, keepdims=True)
        scaled = (centered * lax.rsqrt(variance + EPSILON)).T
        tri_normed = (scaled * out_gain_ref[...] + out_bias_ref[...]).astype(jnp.bfloat16)
        mixed = jnp.dot(tri_normed, out_weight_ref[...], preferred_element_type=jnp.float32)
        out_ref[q * per_tile : (q + 1) * per_tile] = (
            (gating_ref[lanes, :] * mixed).astype(jnp.bfloat16).reshape(per_tile, width, channels)
        )

    for copies in (right_copies, left_copies, tri_copies):
        for copy in copies:
            copy.wait_send()
    for t in range(nx - 1):
        for piece in range(PIECES):
            for way in range(2):

                @pl.when(jnp.logical_and(has_ahead(way), has_origin(way, t)))
                def _():
                    pass_on(way, t, piece).wait_send()


def fused(nx, ny, nz, *arguments):
    pair, pair_mask, in_gain, in_bias, proj_weight, gate_weight, out_gain, out_bias, out_weight = arguments
    rows, width, channels = pair.shape
    hidden = proj_weight.shape[1] // 4
    plane = ny * nz
    block = hidden // plane
    tiles = rows * width // LANES
    travelling = pltpu.VMEM((plane, tiles, block, LANES), jnp.bfloat16)
    return pl.pallas_call(
        functools.partial(kernel, nx, ny, nz),
        out_shape=jax.ShapeDtypeStruct(pair.shape, jnp.bfloat16),
        in_specs=[pl.BlockSpec(memory_space=pltpu.VMEM)] * 9,
        out_specs=pl.BlockSpec(memory_space=pltpu.VMEM),
        scratch_shapes=[travelling] * 6
        + [
            pltpu.VMEM((nx, block, rows, LANES), jnp.bfloat16),
            pltpu.VMEM((block, rows, LANES), jnp.bfloat16),
            pltpu.VMEM((block * rows, LANES), jnp.float32),
            pltpu.VMEM((rows * width, channels), jnp.bfloat16),
            pltpu.VMEM((rows * width, channels), jnp.float32),
        ]
        + [pltpu.SemaphoreType.DMA((2, plane))] * 3
        + [pltpu.SemaphoreType.DMA((2, nx - 1, PIECES))] * 2,
        compiler_params=pltpu.CompilerParams(collective_id=0, has_side_effects=True),
    )(
        pair,
        pair_mask,
        in_gain.reshape(1, -1),
        in_bias.reshape(1, -1),
        proj_weight,
        gate_weight,
        out_gain.reshape(1, -1),
        out_bias.reshape(1, -1),
        out_weight,
    )


def solution(mesh):
    nx, ny, nz = mesh.shape["gx"], mesh.shape["gy"], mesh.shape["gz"]
    plane = ny * nz

    def on_device(pair, *others):
        rows, width, channels = pair.shape
        hidden = others[3].shape[1] // 4
        fits = (
            width * plane == LANES
            and rows * nx == LANES
            and rows % plane == 0
            and channels % LANES == 0
            and hidden % (16 * plane) == 0
        )
        if fits:
            return fused(nx, ny, nz, pair, *others)
        return with_collectives(pair, *others)

    return jax.shard_map(
        on_device,
        mesh=mesh,
        in_specs=(
            P("gx", ("gy", "gz"), None),
            P("gx", ("gy", "gz")),
            P(),
            P(),
            P(),
            P(),
            P(),
            P(),
            P(),
        ),
        out_specs=P("gx", ("gy", "gz"), None),
        check_vma=False,
    )
```

```python
import functools

import jax
import jax.numpy as jnp
from jax import lax
from jax.experimental import pallas as pl
from jax.experimental.pallas import tpu as pltpu
from jax.sharding import PartitionSpec as P

MESH = pl.DeviceIdType.MESH
LANES = 128
EPSILON = 1e-05
PIECES = 4


def normalize(values, gain, bias):
    average = jnp.mean(values, axis=-1, keepdims=True)
    centered = values - average
    variance = jnp.mean(centered * centered, axis=-1, keepdims=True)
    return centered * lax.rsqrt(variance + EPSILON) * gain + bias


def project(tile, mask_value, in_gain, in_bias, proj_weight):
    hidden = proj_weight.shape[1] // 4
    normed = normalize(tile.astype(jnp.float32), in_gain, in_bias).astype(jnp.bfloat16)
    projected = jnp.einsum("rwc,cd->rwd", normed, proj_weight, preferred_element_type=jnp.float32)
    left_side = (
        jax.nn.sigmoid(projected[:, :, :hidden]) * projected[:, :, hidden : 2 * hidden] * mask_value
    ).astype(jnp.bfloat16)
    right_side = (
        jax.nn.sigmoid(projected[:, :, 2 * hidden : 3 * hidden])
        * projected[:, :, 3 * hidden :]
        * mask_value
    ).astype(jnp.bfloat16)
    return (normed, left_side, right_side)


def with_collectives(
    pair, pair_mask, in_gain, in_bias, proj_weight, gate_weight, out_gain, out_bias, out_weight
):
    mask_value = pair_mask.astype(jnp.float32)[:, :, None]
    normed, left_side, own_right = project(pair, mask_value, in_gain, in_bias, proj_weight)
    left_slab, right_slab = (
        lax.all_gather(left_side, "gy", axis=1, tiled=True),
        lax.all_gather(own_right, "gy", axis=1, tiled=True),
    )
    every_row = lax.all_gather(own_right, "gx", axis=0, tiled=True)
    row_panel = lax.all_to_all(every_row, "gy", split_axis=0, concat_axis=1, tiled=True)
    summed = lax.psum_scatter(
        jnp.einsum("jkc,ikc->jic", row_panel, left_slab, preferred_element_type=jnp.float32),
        "gz",
        scatter_dimension=0,
        tiled=True,
    )
    triangle = jnp.transpose(summed, (1, 0, 2))
    tri_normed = normalize(triangle, out_gain, out_bias).astype(jnp.bfloat16)
    gating = jax.nn.sigmoid(
        jnp.einsum("rwc,cd->rwd", normed, gate_weight, preferred_element_type=jnp.float32)
    )
    mixed = jnp.einsum("rwh,hc->rwc", tri_normed, out_weight, preferred_element_type=jnp.float32)
    return (gating * mixed).astype(jnp.bfloat16)


def swap_groups(tiles, width):
    tiles = list(tiles)
    group = lax.broadcasted_iota(jnp.int32, tiles[0].shape, 1) // width
    bit = 1
    while bit < len(tiles):
        upper = (group // bit) % 2 == 1
        for a in range(len(tiles)):
            if (a // bit) % 2 == 0:
                low, high = tiles[a], tiles[a + bit]
                tiles[a] = jnp.where(upper, pltpu.roll(high, bit * width, 1), low)
                tiles[a + bit] = jnp.where(upper, high, pltpu.roll(low, LANES - bit * width, 1))
        bit *= 2
    return tiles


def kernel(
    nx,
    ny,
    nz,
    pair_ref,
    mask_ref,
    in_gain_ref,
    in_bias_ref,
    proj_ref,
    gate_ref,
    out_gain_ref,
    out_bias_ref,
    out_weight_ref,
    out_ref,
    right_out,
    left_out,
    tri_out,
    right_in,
    left_in,
    tri_in,
    right_all,
    left_all,
    left_far,
    tri_far,
    spread,
    normed_ref,
    gating_ref,
    right_sems,
    left_sems,
    tri_sems,
    z_send,
    z_recv,
    far_sems,
    far_send,
):
    rows, width, channels = pair_ref.shape
    hidden = proj_ref.shape[1] // 4
    plane = ny * nz
    block = hidden // plane
    tiles = rows * width // LANES
    per_tile = rows // tiles
    part = block // PIECES
    x, y, z = lax.axis_index("gx"), lax.axis_index("gy"), lax.axis_index("gz")
    me = y * nz + z
    owners = rows // width
    is_end = jnp.logical_or(x == 0, x == nx - 1)
    is_helper = jnp.logical_or(x == 1, x == nx - 2)
    end = jnp.where(x < nx // 2, 0, nx - 1)
    helper = jnp.where(x < nx // 2, 1, nx - 2)

    def is_left_out(d):
        return jnp.logical_and(is_end, d // owners == nx - 1 - end)


    def peer(t):
        d = lax.rem(me + t, plane)
        return d, (x, d // nz, lax.rem(d, nz))

    barrier = pltpu.get_barrier_semaphore()
    for t in range(1, plane):
        pl.semaphore_signal(barrier, inc=1, device_id=peer(t)[1], device_id_type=MESH)

    @pl.when(x > 0)
    def _():
        pl.semaphore_signal(barrier, inc=1, device_id=(x - 1, y, z), device_id_type=MESH)

    @pl.when(x < nx - 1)
    def _():
        pl.semaphore_signal(barrier, inc=1, device_id=(x + 1, y, z), device_id_type=MESH)

    @pl.when(is_left_out(me))
    def _():
        for t in range(plane):
            d = lax.rem(me + t, plane)
            device = (helper, d // nz, lax.rem(d, nz))
            pl.semaphore_signal(barrier, inc=1, device_id=device, device_id_type=MESH)

    normed = normalize(
        pair_ref[...].reshape(rows * width, channels).astype(jnp.float32),
        in_gain_ref[...],
        in_bias_ref[...],
    ).astype(jnp.bfloat16)
    normed_ref[...] = normed

    row_of = lax.broadcasted_iota(jnp.int32, (rows, rows * width), 1) // width
    choose = (row_of == lax.broadcasted_iota(jnp.int32, row_of.shape, 0)).astype(jnp.bfloat16)
    repeated = jnp.dot(
        mask_ref[...].astype(jnp.float32).astype(jnp.bfloat16), choose, preferred_element_type=jnp.float32
    )
    column_of = lax.broadcasted_iota(jnp.int32, repeated.shape, 1) % width
    own_column = column_of == lax.broadcasted_iota(jnp.int32, repeated.shape, 0)
    mask_row = jnp.sum(jnp.where(own_column, repeated, 0.0), axis=0, keepdims=True)

    def side(first, target):
        weight = proj_ref[:, first : first + 2 * hidden].T
        for q in range(tiles):
            lanes = slice(q * LANES, (q + 1) * LANES)
            projected = lax.dot_general(
                weight, normed_ref[lanes, :], (((1,), (1,)), ((), ())), preferred_element_type=jnp.float32
            )
            value = jax.nn.sigmoid(projected[:hidden]) * projected[hidden:] * mask_row[:, lanes]
            target[:, q] = value.astype(jnp.bfloat16).reshape(plane, block, LANES)

    def exchange(source, target, sems):
        copies = []
        for t in range(1, plane):
            d, device = peer(t)
            copies.append(
                pltpu.make_async_remote_copy(
                    src_ref=source.at[d],
                    dst_ref=target.at[me],
                    send_sem=sems.at[0, t],
                    recv_sem=sems.at[1, t],
                    device_id=device,
                    device_id_type=MESH,
                )
            )
            copies[-1].start()
        return copies

    def gather_sums(source, target):
        for q in range(tiles):
            swapped = swap_groups([source[a, q].astype(jnp.float32) for a in range(plane)], width)
            for a in range(per_tile):
                spread[pl.ds(q * per_tile + a, block, stride=rows), :] = swapped[a]
        target[...] = spread[...].astype(jnp.bfloat16).reshape(block, rows, LANES)

    side(2 * hidden, right_out)
    pl.semaphore_wait(
        barrier, jnp.where(is_end, plane, jnp.where(is_helper, plane + 1 + owners, plane + 1))
    )
    right_copies = exchange(right_out, right_in, right_sems)
    right_in[me] = right_out[me]
    side(0, left_out)
    left_copies = exchange(left_out, left_in, left_sems)
    left_in[me] = left_out[me]
    gating_ref[...] = jax.nn.sigmoid(
        jnp.dot(normed_ref[...], gate_ref[...], preferred_element_type=jnp.float32)
    )

    for copy in right_copies:
        copy.wait_recv()
    gather_sums(right_in, right_all.at[x])

    def pass_on(way, t, piece):
        ahead = x + 1 if way == 0 else x - 1
        origin = x - t if way == 0 else x + t
        part_of = right_all.at[origin, pl.ds(piece * part, part)]
        return pltpu.make_async_remote_copy(
            src_ref=part_of,
            dst_ref=part_of,
            send_sem=z_send.at[way, t, piece],
            recv_sem=z_recv.at[way, t, piece],
            device_id=(ahead, y, z),
            device_id_type=MESH,
        )

    def has_ahead(way):
        return x < nx - 1 if way == 0 else x > 0

    def has_origin(way, t):
        return x >= t if way == 0 else x <= nx - 1 - t

    for piece in range(PIECES):
        for way in range(2):

            @pl.when(has_ahead(way))
            def _():
                pass_on(way, 0, piece).start()

    for copy in left_copies:
        copy.wait_recv()
    gather_sums(left_in, left_all)

    left_copy = pltpu.make_async_remote_copy(
        src_ref=left_all,
        dst_ref=left_far,
        send_sem=far_sems.at[0],
        recv_sem=far_sems.at[1],
        device_id=(helper, y, z),
        device_id_type=MESH,
    )

    @pl.when(is_end)
    def _():
        left_copy.start()
        right_all[nx - 1 - end] = jnp.zeros(right_all.shape[1:], right_all.dtype)

    for t in range(1, nx - 1):
        for piece in range(PIECES):
            for way in range(2):

                @pl.when(has_origin(way, t))
                def _():
                    pltpu.make_async_remote_copy(
                        src_ref=right_all.at[x, pl.ds(piece * part, part)],
                        dst_ref=right_all.at[x - t if way == 0 else x + t, pl.ds(piece * part, part)],
                        send_sem=z_send.at[way, t - 1, piece],
                        recv_sem=z_recv.at[way, t - 1, piece],
                        device_id=(x, y, z),
                        device_id_type=MESH,
                    ).wait_recv()
                    if t < nx - 2:

                        @pl.when(has_ahead(way))
                        def _():
                            pass_on(way, t, piece).start()

    def multiply(left, target):
        for c in range(block):
            triangle = lax.dot_general(
                left[c],
                right_all[:, c].reshape(nx * rows, LANES),
                (((1,), (1,)), ((), ())),
                preferred_element_type=jnp.float32,
            )
            spread[pl.ds(c, rows, stride=block), :] = triangle
        for q in range(tiles):
            swapped = swap_groups(
                [spread[pl.ds((q * per_tile + a) * block, block), :] for a in range(per_tile)], width
            )
            for d in range(plane):
                target[d, q] = swapped[d].astype(jnp.bfloat16)

    def far_copy(index):
        d = (nx - 1 - end) * owners + index
        return pltpu.make_async_remote_copy(
            src_ref=tri_far.at[d],
            dst_ref=tri_in.at[me],
            send_sem=far_send.at[index],
            recv_sem=tri_sems.at[1, lax.rem(d - me + plane, plane)],
            device_id=(end, d // nz, lax.rem(d, nz)),
            device_id_type=MESH,
        )

    def tri_copy(t):
        d, device = peer(t)
        return pltpu.make_async_remote_copy(
            src_ref=tri_out.at[d],
            dst_ref=tri_in.at[me],
            send_sem=tri_sems.at[0, t],
            recv_sem=tri_sems.at[1, t],
            device_id=device,
            device_id_type=MESH,
        )

    @pl.when(is_helper)
    def _():
        left_copy.wait_recv()
        multiply(left_far, tri_far)
        for index in range(owners):
            far_copy(index).start()

    multiply(left_all, tri_out)
    for t in range(1, plane):

        @pl.when(jnp.logical_not(is_left_out(peer(t)[0])))
        def _():
            tri_copy(t).start()

    @pl.when(jnp.logical_not(is_left_out(me)))
    def _():
        tri_in[me] = tri_out[me]

    @pl.when(is_left_out(me))
    def _():
        tri_copy(0).wait_recv()

    for t in range(1, plane):
        tri_copy(t).wait_recv()

    for q in range(tiles):
        lanes = slice(q * LANES, (q + 1) * LANES)
        sums = tri_in[:, q].reshape(hidden, LANES).astype(jnp.float32)
        centered = sums - jnp.mean(sums, axis=0, keepdims=True)
        variance = jnp.mean(centered * centered, axis=0, keepdims=True)
        scaled = (centered * lax.rsqrt(variance + EPSILON)).T
        tri_normed = (scaled * out_gain_ref[...] + out_bias_ref[...]).astype(jnp.bfloat16)
        mixed = jnp.dot(tri_normed, out_weight_ref[...], preferred_element_type=jnp.float32)
        out_ref[q * per_tile : (q + 1) * per_tile] = (
            (gating_ref[lanes, :] * mixed).astype(jnp.bfloat16).reshape(per_tile, width, channels)
        )

    for copy in right_copies + left_copies:
        copy.wait_send()
    for t in range(1, plane):

        @pl.when(jnp.logical_not(is_left_out(peer(t)[0])))
        def _():
            tri_copy(t).wait_send()

    @pl.when(is_helper)
    def _():
        for index in range(owners):
            far_copy(index).wait_send()

    @pl.when(is_end)
    def _():
        left_copy.wait_send()

    for t in range(nx - 2):
        for piece in range(PIECES):
            for way in range(2):

                @pl.when(jnp.logical_and(has_ahead(way), has_origin(way, t)))
                def _():
                    pass_on(way, t, piece).wait_send()


def fused(nx, ny, nz, *arguments):
    pair, pair_mask, in_gain, in_bias, proj_weight, gate_weight, out_gain, out_bias, out_weight = arguments
    rows, width, channels = pair.shape
    hidden = proj_weight.shape[1] // 4
    plane = ny * nz
    block = hidden // plane
    tiles = rows * width // LANES
    travelling = pltpu.VMEM((plane, tiles, block, LANES), jnp.bfloat16)
    return pl.pallas_call(
        functools.partial(kernel, nx, ny, nz),
        out_shape=jax.ShapeDtypeStruct(pair.shape, jnp.bfloat16),
        in_specs=[pl.BlockSpec(memory_space=pltpu.VMEM)] * 9,
        out_specs=pl.BlockSpec(memory_space=pltpu.VMEM),
        scratch_shapes=[travelling] * 6
        + [
            pltpu.VMEM((nx, block, rows, LANES), jnp.bfloat16),
            pltpu.VMEM((block, rows, LANES), jnp.bfloat16),
            pltpu.VMEM((block, rows, LANES), jnp.bfloat16),
            travelling,
            pltpu.VMEM((block * rows, LANES), jnp.float32),
            pltpu.VMEM((rows * width, channels), jnp.bfloat16),
            pltpu.VMEM((rows * width, channels), jnp.float32),
        ]
        + [pltpu.SemaphoreType.DMA((2, plane))] * 3
        + [pltpu.SemaphoreType.DMA((2, nx - 2, PIECES))] * 2
        + [pltpu.SemaphoreType.DMA((2,)), pltpu.SemaphoreType.DMA((rows // width,))],
        compiler_params=pltpu.CompilerParams(collective_id=0, has_side_effects=True),
    )(
        pair,
        pair_mask.T,
        in_gain.reshape(1, -1),
        in_bias.reshape(1, -1),
        proj_weight,
        gate_weight,
        out_gain.reshape(1, -1),
        out_bias.reshape(1, -1),
        out_weight,
    )


def solution(mesh):
    nx, ny, nz = mesh.shape["gx"], mesh.shape["gy"], mesh.shape["gz"]
    plane = ny * nz

    def on_device(pair, *others):
        rows, width, channels = pair.shape
        hidden = others[3].shape[1] // 4
        fits = (
            width * plane == LANES
            and rows * nx == LANES
            and rows % plane == 0
            and rows % width == 0
            and nx >= 4
            and channels % LANES == 0
            and hidden % (16 * plane) == 0
        )
        if fits:
            return fused(nx, ny, nz, pair, *others)
        return with_collectives(pair, *others)

    return jax.shard_map(
        on_device,
        mesh=mesh,
        in_specs=(
            P("gx", ("gy", "gz"), None),
            P("gx", ("gy", "gz")),
            P(),
            P(),
            P(),
            P(),
            P(),
            P(),
            P(),
        ),
        out_specs=P("gx", ("gy", "gz"), None),
        check_vma=False,
    )
```

```python
import functools

import jax
import jax.numpy as jnp
from jax import lax
from jax.experimental import pallas as pl
from jax.experimental.pallas import tpu as pltpu
from jax.sharding import PartitionSpec as P

MESH = pl.DeviceIdType.MESH
LANES = 128
EPSILON = 1e-05
PIECES = 4


def normalize(values, gain, bias):
    average = jnp.mean(values, axis=-1, keepdims=True)
    centered = values - average
    variance = jnp.mean(centered * centered, axis=-1, keepdims=True)
    return centered * lax.rsqrt(variance + EPSILON) * gain + bias


def project(tile, mask_value, in_gain, in_bias, proj_weight):
    hidden = proj_weight.shape[1] // 4
    normed = normalize(tile.astype(jnp.float32), in_gain, in_bias).astype(jnp.bfloat16)
    projected = jnp.einsum("rwc,cd->rwd", normed, proj_weight, preferred_element_type=jnp.float32)
    left_side = (
        jax.nn.sigmoid(projected[:, :, :hidden]) * projected[:, :, hidden : 2 * hidden] * mask_value
    ).astype(jnp.bfloat16)
    right_side = (
        jax.nn.sigmoid(projected[:, :, 2 * hidden : 3 * hidden])
        * projected[:, :, 3 * hidden :]
        * mask_value
    ).astype(jnp.bfloat16)
    return (normed, left_side, right_side)


def with_collectives(
    pair, pair_mask, in_gain, in_bias, proj_weight, gate_weight, out_gain, out_bias, out_weight
):
    mask_value = pair_mask.astype(jnp.float32)[:, :, None]
    normed, left_side, own_right = project(pair, mask_value, in_gain, in_bias, proj_weight)
    left_slab, right_slab = (
        lax.all_gather(left_side, "gy", axis=1, tiled=True),
        lax.all_gather(own_right, "gy", axis=1, tiled=True),
    )
    every_row = lax.all_gather(own_right, "gx", axis=0, tiled=True)
    row_panel = lax.all_to_all(every_row, "gy", split_axis=0, concat_axis=1, tiled=True)
    summed = lax.psum_scatter(
        jnp.einsum("jkc,ikc->jic", row_panel, left_slab, preferred_element_type=jnp.float32),
        "gz",
        scatter_dimension=0,
        tiled=True,
    )
    triangle = jnp.transpose(summed, (1, 0, 2))
    tri_normed = normalize(triangle, out_gain, out_bias).astype(jnp.bfloat16)
    gating = jax.nn.sigmoid(
        jnp.einsum("rwc,cd->rwd", normed, gate_weight, preferred_element_type=jnp.float32)
    )
    mixed = jnp.einsum("rwh,hc->rwc", tri_normed, out_weight, preferred_element_type=jnp.float32)
    return (gating * mixed).astype(jnp.bfloat16)


def swap_groups(tiles, width):
    tiles = list(tiles)
    group = lax.broadcasted_iota(jnp.int32, tiles[0].shape, 1) // width
    bit = 1
    while bit < len(tiles):
        upper = (group // bit) % 2 == 1
        for a in range(len(tiles)):
            if (a // bit) % 2 == 0:
                low, high = tiles[a], tiles[a + bit]
                tiles[a] = jnp.where(upper, pltpu.roll(high, bit * width, 1), low)
                tiles[a + bit] = jnp.where(upper, high, pltpu.roll(low, LANES - bit * width, 1))
        bit *= 2
    return tiles


def kernel(
    nx,
    ny,
    nz,
    pair_hbm,
    mask_hbm,
    in_gain_hbm,
    in_bias_hbm,
    proj_hbm,
    gate_hbm,
    out_gain_hbm,
    out_bias_hbm,
    out_weight_hbm,
    out_ref,
    right_out,
    left_out,
    tri_out,
    right_in,
    left_in,
    tri_in,
    right_all,
    left_all,
    left_far,
    tri_far,
    spread,
    normed_ref,
    gating_ref,
    right_sems,
    left_sems,
    tri_sems,
    z_send,
    z_recv,
    far_sems,
    far_send,
    pair_ref,
    mask_ref,
    in_gain_ref,
    in_bias_ref,
    proj_ref,
    gate_ref,
    out_gain_ref,
    out_bias_ref,
    out_weight_ref,
    load_sems,
):
    rows, width, channels = pair_ref.shape
    hidden = proj_ref.shape[1] // 4
    plane = ny * nz
    block = hidden // plane
    tiles = rows * width // LANES
    per_tile = rows // tiles
    part = block // PIECES
    x, y, z = lax.axis_index("gx"), lax.axis_index("gy"), lax.axis_index("gz")
    me = y * nz + z
    owners = rows // width
    is_end = jnp.logical_or(x == 0, x == nx - 1)
    is_helper = jnp.logical_or(x == 1, x == nx - 2)
    end = jnp.where(x < nx // 2, 0, nx - 1)
    helper = jnp.where(x < nx // 2, 1, nx - 2)

    def is_left_out(d):
        return jnp.logical_and(is_end, d // owners == nx - 1 - end)


    def peer(t):
        d = lax.rem(me + t, plane)
        return d, (x, d // nz, lax.rem(d, nz))

    arguments = (
        (pair_hbm, pair_ref),
        (mask_hbm, mask_ref),
        (in_gain_hbm, in_gain_ref),
        (in_bias_hbm, in_bias_ref),
        (proj_hbm, proj_ref),
        (gate_hbm, gate_ref),
        (out_gain_hbm, out_gain_ref),
        (out_bias_hbm, out_bias_ref),
        (out_weight_hbm, out_weight_ref),
    )
    loads = [
        pltpu.make_async_copy(held, wanted, load_sems.at[index])
        for index, (held, wanted) in enumerate(arguments)
    ]
    for load in loads:
        load.start()
    barrier = pltpu.get_barrier_semaphore()
    for t in range(1, plane):
        pl.semaphore_signal(barrier, inc=1, device_id=peer(t)[1], device_id_type=MESH)

    @pl.when(x > 0)
    def _():
        pl.semaphore_signal(barrier, inc=1, device_id=(x - 1, y, z), device_id_type=MESH)

    @pl.when(x < nx - 1)
    def _():
        pl.semaphore_signal(barrier, inc=1, device_id=(x + 1, y, z), device_id_type=MESH)

    @pl.when(is_left_out(me))
    def _():
        for t in range(plane):
            d = lax.rem(me + t, plane)
            device = (helper, d // nz, lax.rem(d, nz))
            pl.semaphore_signal(barrier, inc=1, device_id=device, device_id_type=MESH)

    for load in (loads[0], loads[2], loads[3]):
        load.wait()
    normed = normalize(
        pair_ref[...].reshape(rows * width, channels).astype(jnp.float32),
        in_gain_ref[...],
        in_bias_ref[...],
    ).astype(jnp.bfloat16)
    normed_ref[...] = normed

    loads[1].wait()
    row_of = lax.broadcasted_iota(jnp.int32, (rows, rows * width), 1) // width
    choose = (row_of == lax.broadcasted_iota(jnp.int32, row_of.shape, 0)).astype(jnp.bfloat16)
    repeated = jnp.dot(
        mask_ref[...].astype(jnp.float32).astype(jnp.bfloat16), choose, preferred_element_type=jnp.float32
    )
    column_of = lax.broadcasted_iota(jnp.int32, repeated.shape, 1) % width
    own_column = column_of == lax.broadcasted_iota(jnp.int32, repeated.shape, 0)
    mask_row = jnp.sum(jnp.where(own_column, repeated, 0.0), axis=0, keepdims=True)

    def side(first, target):
        weight = proj_ref[:, first : first + 2 * hidden].T
        for q in range(tiles):
            lanes = slice(q * LANES, (q + 1) * LANES)
            projected = lax.dot_general(
                weight, normed_ref[lanes, :], (((1,), (1,)), ((), ())), preferred_element_type=jnp.float32
            )
            value = jax.nn.sigmoid(projected[:hidden]) * projected[hidden:] * mask_row[:, lanes]
            target[:, q] = value.astype(jnp.bfloat16).reshape(plane, block, LANES)

    def exchange(source, target, sems):
        copies = []
        for t in range(1, plane):
            d, device = peer(t)
            copies.append(
                pltpu.make_async_remote_copy(
                    src_ref=source.at[d],
                    dst_ref=target.at[me],
                    send_sem=sems.at[0, t],
                    recv_sem=sems.at[1, t],
                    device_id=device,
                    device_id_type=MESH,
                )
            )
            copies[-1].start()
        return copies

    def gather_sums(source, target):
        for q in range(tiles):
            swapped = swap_groups([source[a, q].astype(jnp.float32) for a in range(plane)], width)
            for a in range(per_tile):
                spread[pl.ds(q * per_tile + a, block, stride=rows), :] = swapped[a]
        target[...] = spread[...].astype(jnp.bfloat16).reshape(block, rows, LANES)

    loads[4].wait()
    side(2 * hidden, right_out)
    pl.semaphore_wait(
        barrier, jnp.where(is_end, plane, jnp.where(is_helper, plane + 1 + owners, plane + 1))
    )
    right_copies = exchange(right_out, right_in, right_sems)
    right_in[me] = right_out[me]
    side(0, left_out)
    left_copies = exchange(left_out, left_in, left_sems)
    left_in[me] = left_out[me]
    loads[5].wait()
    gating_ref[...] = jax.nn.sigmoid(
        jnp.dot(normed_ref[...], gate_ref[...], preferred_element_type=jnp.float32)
    )

    for copy in right_copies:
        copy.wait_recv()
    gather_sums(right_in, right_all.at[x])

    def pass_on(way, t, piece):
        ahead = x + 1 if way == 0 else x - 1
        origin = x - t if way == 0 else x + t
        part_of = right_all.at[origin, pl.ds(piece * part, part)]
        return pltpu.make_async_remote_copy(
            src_ref=part_of,
            dst_ref=part_of,
            send_sem=z_send.at[way, t, piece],
            recv_sem=z_recv.at[way, t, piece],
            device_id=(ahead, y, z),
            device_id_type=MESH,
        )

    def has_ahead(way):
        return x < nx - 1 if way == 0 else x > 0

    def has_origin(way, t):
        return x >= t if way == 0 else x <= nx - 1 - t

    for piece in range(PIECES):
        for way in range(2):

            @pl.when(has_ahead(way))
            def _():
                pass_on(way, 0, piece).start()

    for copy in left_copies:
        copy.wait_recv()
    gather_sums(left_in, left_all)

    left_copy = pltpu.make_async_remote_copy(
        src_ref=left_all,
        dst_ref=left_far,
        send_sem=far_sems.at[0],
        recv_sem=far_sems.at[1],
        device_id=(helper, y, z),
        device_id_type=MESH,
    )

    @pl.when(is_end)
    def _():
        left_copy.start()
        right_all[nx - 1 - end] = jnp.zeros(right_all.shape[1:], right_all.dtype)

    for t in range(1, nx - 1):
        for piece in range(PIECES):
            for way in range(2):

                @pl.when(has_origin(way, t))
                def _():
                    pltpu.make_async_remote_copy(
                        src_ref=right_all.at[x, pl.ds(piece * part, part)],
                        dst_ref=right_all.at[x - t if way == 0 else x + t, pl.ds(piece * part, part)],
                        send_sem=z_send.at[way, t - 1, piece],
                        recv_sem=z_recv.at[way, t - 1, piece],
                        device_id=(x, y, z),
                        device_id_type=MESH,
                    ).wait_recv()
                    if t < nx - 2:

                        @pl.when(has_ahead(way))
                        def _():
                            pass_on(way, t, piece).start()

    def multiply(left, target):
        for c in range(block):
            triangle = lax.dot_general(
                left[c],
                right_all[:, c].reshape(nx * rows, LANES),
                (((1,), (1,)), ((), ())),
                preferred_element_type=jnp.float32,
            )
            spread[pl.ds(c, rows, stride=block), :] = triangle
        for q in range(tiles):
            swapped = swap_groups(
                [spread[pl.ds((q * per_tile + a) * block, block), :] for a in range(per_tile)], width
            )
            for d in range(plane):
                target[d, q] = swapped[d].astype(jnp.bfloat16)

    def far_copy(index):
        d = (nx - 1 - end) * owners + index
        return pltpu.make_async_remote_copy(
            src_ref=tri_far.at[d],
            dst_ref=tri_in.at[me],
            send_sem=far_send.at[index],
            recv_sem=tri_sems.at[1, lax.rem(d - me + plane, plane)],
            device_id=(end, d // nz, lax.rem(d, nz)),
            device_id_type=MESH,
        )

    def tri_copy(t):
        d, device = peer(t)
        return pltpu.make_async_remote_copy(
            src_ref=tri_out.at[d],
            dst_ref=tri_in.at[me],
            send_sem=tri_sems.at[0, t],
            recv_sem=tri_sems.at[1, t],
            device_id=device,
            device_id_type=MESH,
        )

    @pl.when(is_helper)
    def _():
        left_copy.wait_recv()
        multiply(left_far, tri_far)
        for index in range(owners):
            far_copy(index).start()

    multiply(left_all, tri_out)
    for t in range(1, plane):

        @pl.when(jnp.logical_not(is_left_out(peer(t)[0])))
        def _():
            tri_copy(t).start()

    @pl.when(jnp.logical_not(is_left_out(me)))
    def _():
        tri_in[me] = tri_out[me]

    @pl.when(is_left_out(me))
    def _():
        tri_copy(0).wait_recv()

    for t in range(1, plane):
        tri_copy(t).wait_recv()

    for load in loads[6:]:
        load.wait()
    for q in range(tiles):
        lanes = slice(q * LANES, (q + 1) * LANES)
        sums = tri_in[:, q].reshape(hidden, LANES).astype(jnp.float32)
        centered = sums - jnp.mean(sums, axis=0, keepdims=True)
        variance = jnp.mean(centered * centered, axis=0, keepdims=True)
        scaled = (centered * lax.rsqrt(variance + EPSILON)).T
        tri_normed = (scaled * out_gain_ref[...] + out_bias_ref[...]).astype(jnp.bfloat16)
        mixed = jnp.dot(tri_normed, out_weight_ref[...], preferred_element_type=jnp.float32)
        out_ref[q * per_tile : (q + 1) * per_tile] = (
            (gating_ref[lanes, :] * mixed).astype(jnp.bfloat16).reshape(per_tile, width, channels)
        )

    for copy in right_copies + left_copies:
        copy.wait_send()
    for t in range(1, plane):

        @pl.when(jnp.logical_not(is_left_out(peer(t)[0])))
        def _():
            tri_copy(t).wait_send()

    @pl.when(is_helper)
    def _():
        for index in range(owners):
            far_copy(index).wait_send()

    @pl.when(is_end)
    def _():
        left_copy.wait_send()

    for t in range(nx - 2):
        for piece in range(PIECES):
            for way in range(2):

                @pl.when(jnp.logical_and(has_ahead(way), has_origin(way, t)))
                def _():
                    pass_on(way, t, piece).wait_send()


def fused(nx, ny, nz, *arguments):
    pair, pair_mask, in_gain, in_bias, proj_weight, gate_weight, out_gain, out_bias, out_weight = arguments
    rows, width, channels = pair.shape
    hidden = proj_weight.shape[1] // 4
    plane = ny * nz
    block = hidden // plane
    tiles = rows * width // LANES
    travelling = pltpu.VMEM((plane, tiles, block, LANES), jnp.bfloat16)
    return pl.pallas_call(
        functools.partial(kernel, nx, ny, nz),
        out_shape=jax.ShapeDtypeStruct(pair.shape, jnp.bfloat16),
        in_specs=[pl.BlockSpec(memory_space=pltpu.HBM)] * 9,
        out_specs=pl.BlockSpec(memory_space=pltpu.VMEM),
        scratch_shapes=[travelling] * 6
        + [
            pltpu.VMEM((nx, block, rows, LANES), jnp.bfloat16),
            pltpu.VMEM((block, rows, LANES), jnp.bfloat16),
            pltpu.VMEM((block, rows, LANES), jnp.bfloat16),
            travelling,
            pltpu.VMEM((block * rows, LANES), jnp.float32),
            pltpu.VMEM((rows * width, channels), jnp.bfloat16),
            pltpu.VMEM((rows * width, channels), jnp.float32),
        ]
        + [pltpu.SemaphoreType.DMA((2, plane))] * 3
        + [pltpu.SemaphoreType.DMA((2, nx - 2, PIECES))] * 2
        + [pltpu.SemaphoreType.DMA((2,)), pltpu.SemaphoreType.DMA((rows // width,))]
        + [
            pltpu.VMEM(pair.shape, pair.dtype),
            pltpu.VMEM((width, rows), pair_mask.dtype),
            pltpu.VMEM((1, in_gain.size), in_gain.dtype),
            pltpu.VMEM((1, in_bias.size), in_bias.dtype),
            pltpu.VMEM(proj_weight.shape, proj_weight.dtype),
            pltpu.VMEM(gate_weight.shape, gate_weight.dtype),
            pltpu.VMEM((1, out_gain.size), out_gain.dtype),
            pltpu.VMEM((1, out_bias.size), out_bias.dtype),
            pltpu.VMEM(out_weight.shape, out_weight.dtype),
            pltpu.SemaphoreType.DMA((9,)),
        ],
        compiler_params=pltpu.CompilerParams(collective_id=0, has_side_effects=True),
    )(
        pair,
        pair_mask.T,
        in_gain.reshape(1, -1),
        in_bias.reshape(1, -1),
        proj_weight,
        gate_weight,
        out_gain.reshape(1, -1),
        out_bias.reshape(1, -1),
        out_weight,
    )


def solution(mesh):
    nx, ny, nz = mesh.shape["gx"], mesh.shape["gy"], mesh.shape["gz"]
    plane = ny * nz

    def on_device(pair, *others):
        rows, width, channels = pair.shape
        hidden = others[3].shape[1] // 4
        fits = (
            width * plane == LANES
            and rows * nx == LANES
            and rows % plane == 0
            and rows % width == 0
            and nx >= 4
            and channels % LANES == 0
            and hidden % (16 * plane) == 0
        )
        if fits:
            return fused(nx, ny, nz, pair, *others)
        return with_collectives(pair, *others)

    return jax.shard_map(
        on_device,
        mesh=mesh,
        in_specs=(
            P("gx", ("gy", "gz"), None),
            P("gx", ("gy", "gz")),
            P(),
            P(),
            P(),
            P(),
            P(),
            P(),
            P(),
        ),
        out_specs=P("gx", ("gy", "gz"), None),
        check_vma=False,
    )
```

```python
import functools

import jax
import jax.numpy as jnp
from jax import lax
from jax.experimental import pallas as pl
from jax.experimental.pallas import tpu as pltpu
from jax.sharding import PartitionSpec as P

MESH = pl.DeviceIdType.MESH
LANES = 128
EPSILON = 1e-05
PARTS = 2
RIGHT_STEPS = 2
TRI_STEPS = 1


def normalize(values, gain, bias):
    average = jnp.mean(values, axis=-1, keepdims=True)
    centered = values - average
    variance = jnp.mean(centered * centered, axis=-1, keepdims=True)
    return centered * lax.rsqrt(variance + EPSILON) * gain + bias


def project(tile, mask_value, in_gain, in_bias, proj_weight):
    hidden = proj_weight.shape[1] // 4
    normed = normalize(tile.astype(jnp.float32), in_gain, in_bias).astype(jnp.bfloat16)
    projected = jnp.einsum("rwc,cd->rwd", normed, proj_weight, preferred_element_type=jnp.float32)
    left_side = (
        jax.nn.sigmoid(projected[:, :, :hidden]) * projected[:, :, hidden : 2 * hidden] * mask_value
    ).astype(jnp.bfloat16)
    right_side = (
        jax.nn.sigmoid(projected[:, :, 2 * hidden : 3 * hidden])
        * projected[:, :, 3 * hidden :]
        * mask_value
    ).astype(jnp.bfloat16)
    return (normed, left_side, right_side)


def with_collectives(
    pair, pair_mask, in_gain, in_bias, proj_weight, gate_weight, out_gain, out_bias, out_weight
):
    mask_value = pair_mask.astype(jnp.float32)[:, :, None]
    normed, left_side, own_right = project(pair, mask_value, in_gain, in_bias, proj_weight)
    left_slab, right_slab = (
        lax.all_gather(left_side, "gy", axis=1, tiled=True),
        lax.all_gather(own_right, "gy", axis=1, tiled=True),
    )
    every_row = lax.all_gather(own_right, "gx", axis=0, tiled=True)
    row_panel = lax.all_to_all(every_row, "gy", split_axis=0, concat_axis=1, tiled=True)
    summed = lax.psum_scatter(
        jnp.einsum("jkc,ikc->jic", row_panel, left_slab, preferred_element_type=jnp.float32),
        "gz",
        scatter_dimension=0,
        tiled=True,
    )
    triangle = jnp.transpose(summed, (1, 0, 2))
    tri_normed = normalize(triangle, out_gain, out_bias).astype(jnp.bfloat16)
    gating = jax.nn.sigmoid(
        jnp.einsum("rwc,cd->rwd", normed, gate_weight, preferred_element_type=jnp.float32)
    )
    mixed = jnp.einsum("rwh,hc->rwc", tri_normed, out_weight, preferred_element_type=jnp.float32)
    return (gating * mixed).astype(jnp.bfloat16)


def swap_groups(tiles, width):
    tiles = list(tiles)
    group = lax.broadcasted_iota(jnp.int32, tiles[0].shape, 1) // width
    bit = 1
    while bit < len(tiles):
        upper = (group // bit) % 2 == 1
        for a in range(len(tiles)):
            if (a // bit) % 2 == 0:
                low, high = tiles[a], tiles[a + bit]
                tiles[a] = jnp.where(upper, pltpu.roll(high, bit * width, 1), low)
                tiles[a + bit] = jnp.where(upper, high, pltpu.roll(low, LANES - bit * width, 1))
        bit *= 2
    return tiles


def kernel(
    nx,
    ny,
    nz,
    pair_hbm,
    mask_hbm,
    in_gain_hbm,
    in_bias_hbm,
    proj_hbm,
    gate_hbm,
    out_gain_hbm,
    out_bias_hbm,
    out_weight_hbm,
    out_ref,
    right_out,
    left_out,
    tri_out,
    right_in,
    left_in,
    tri_in,
    right_all,
    left_all,
    left_far,
    tri_far,
    spread,
    normed_ref,
    gating_ref,
    right_sems,
    left_sems,
    tri_sems,
    z_send,
    z_recv,
    far_sems,
    far_send,
    pair_ref,
    mask_ref,
    in_gain_ref,
    in_bias_ref,
    proj_ref,
    gate_ref,
    out_gain_ref,
    out_bias_ref,
    out_weight_ref,
    load_sems,
):
    rows, width, channels = pair_ref.shape
    hidden = proj_ref.shape[1] // 4
    plane = ny * nz
    block = hidden // plane
    tiles = rows * width // LANES
    per_tile = rows // tiles
    per_step = tiles // TRI_STEPS
    part = block // PARTS
    x, y, z = lax.axis_index("gx"), lax.axis_index("gy"), lax.axis_index("gz")
    me = y * nz + z
    owners = rows // width
    is_end = jnp.logical_or(x == 0, x == nx - 1)
    is_helper = jnp.logical_or(x == 1, x == nx - 2)
    end = jnp.where(x < nx // 2, 0, nx - 1)
    helper = jnp.where(x < nx // 2, 1, nx - 2)

    def is_left_out(d):
        return jnp.logical_and(is_end, d // owners == nx - 1 - end)


    def peer(t):
        d = lax.rem(me + t, plane)
        return d, (x, d // nz, lax.rem(d, nz))

    arguments = (
        (pair_hbm, pair_ref),
        (mask_hbm, mask_ref),
        (in_gain_hbm, in_gain_ref),
        (in_bias_hbm, in_bias_ref),
        (proj_hbm, proj_ref),
        (gate_hbm, gate_ref),
        (out_gain_hbm, out_gain_ref),
        (out_bias_hbm, out_bias_ref),
        (out_weight_hbm, out_weight_ref),
    )
    loads = [
        pltpu.make_async_copy(held, wanted, load_sems.at[index])
        for index, (held, wanted) in enumerate(arguments)
    ]
    for load in loads:
        load.start()
    barrier = pltpu.get_barrier_semaphore()
    for t in range(1, plane):
        pl.semaphore_signal(barrier, inc=1, device_id=peer(t)[1], device_id_type=MESH)

    @pl.when(x > 0)
    def _():
        pl.semaphore_signal(barrier, inc=1, device_id=(x - 1, y, z), device_id_type=MESH)

    @pl.when(x < nx - 1)
    def _():
        pl.semaphore_signal(barrier, inc=1, device_id=(x + 1, y, z), device_id_type=MESH)

    @pl.when(is_left_out(me))
    def _():
        for t in range(plane):
            d = lax.rem(me + t, plane)
            device = (helper, d // nz, lax.rem(d, nz))
            pl.semaphore_signal(barrier, inc=1, device_id=device, device_id_type=MESH)

    for load in (loads[0], loads[2], loads[3]):
        load.wait()

    def norm(step):
        some = slice(step * rows // RIGHT_STEPS, (step + 1) * rows // RIGHT_STEPS)
        pairs = slice(some.start * width, some.stop * width)
        normed_ref[pairs, :] = normalize(
            pair_ref[some].reshape(-1, channels).astype(jnp.float32), in_gain_ref[...], in_bias_ref[...]
        ).astype(jnp.bfloat16)

    norm(0)

    loads[1].wait()
    row_of = lax.broadcasted_iota(jnp.int32, (rows, rows * width), 1) // width
    choose = (row_of == lax.broadcasted_iota(jnp.int32, row_of.shape, 0)).astype(jnp.bfloat16)
    repeated = jnp.dot(
        mask_ref[...].astype(jnp.float32).astype(jnp.bfloat16), choose, preferred_element_type=jnp.float32
    )
    column_of = lax.broadcasted_iota(jnp.int32, repeated.shape, 1) % width
    own_column = column_of == lax.broadcasted_iota(jnp.int32, repeated.shape, 0)
    mask_row = jnp.sum(jnp.where(own_column, repeated, 0.0), axis=0, keepdims=True)

    def side(weight, target, step, steps):
        for q in range(step * tiles // steps, (step + 1) * tiles // steps):
            lanes = slice(q * LANES, (q + 1) * LANES)
            projected = lax.dot_general(
                weight, normed_ref[lanes, :], (((1,), (1,)), ((), ())), preferred_element_type=jnp.float32
            )
            value = jax.nn.sigmoid(projected[:hidden]) * projected[hidden:] * mask_row[:, lanes]
            target[:, q] = value.astype(jnp.bfloat16).reshape(plane, block, LANES)

    def exchange(source, target, sems, step, steps):
        count = tiles // steps
        copies = []
        for t in range(1, plane):
            d, device = peer(t)
            copies.append(
                pltpu.make_async_remote_copy(
                    src_ref=source.at[d, pl.ds(step * count, count)],
                    dst_ref=target.at[me, pl.ds(step * count, count)],
                    send_sem=sems.at[0, step, t],
                    recv_sem=sems.at[1, step, t],
                    device_id=device,
                    device_id_type=MESH,
                )
            )
            copies[-1].start()
        target[me, step * count : (step + 1) * count] = source[me, step * count : (step + 1) * count]
        return copies

    def gather_sums(source, target, step, steps):
        some = rows // steps
        for index, q in enumerate(range(step * tiles // steps, (step + 1) * tiles // steps)):
            swapped = swap_groups([source[a, q].astype(jnp.float32) for a in range(plane)], width)
            for a in range(per_tile):
                first = step * some * block + index * per_tile + a
                spread[pl.ds(first, block, stride=some), :] = swapped[a]
        target[:, step * some : (step + 1) * some] = (
            spread[step * some * block : (step + 1) * some * block]
            .astype(jnp.bfloat16)
            .reshape(block, some, LANES)
        )

    loads[4].wait()
    right_weight = proj_ref[:, 2 * hidden :].T
    right_copies = []
    for step in range(RIGHT_STEPS):
        if step > 0:
            norm(step)
        side(right_weight, right_out, step, RIGHT_STEPS)
        if step == 0:
            pl.semaphore_wait(
                barrier, jnp.where(is_end, plane, jnp.where(is_helper, plane + 1 + owners, plane + 1))
            )
        right_copies.append(exchange(right_out, right_in, right_sems, step, RIGHT_STEPS))
    side(proj_ref[:, : 2 * hidden].T, left_out, 0, 1)
    left_copies = exchange(left_out, left_in, left_sems, 0, 1)
    loads[5].wait()
    gating_ref[...] = jax.nn.sigmoid(
        jnp.dot(normed_ref[...], gate_ref[...], preferred_element_type=jnp.float32)
    )

    pieces = RIGHT_STEPS * PARTS

    def piece_of(origin, piece):
        some = rows // RIGHT_STEPS
        return right_all.at[
            origin, pl.ds(piece % PARTS * part, part), pl.ds(piece // PARTS * some, some)
        ]

    def pass_on(way, t, piece):
        ahead = x + 1 if way == 0 else x - 1
        origin = x - t if way == 0 else x + t
        part_of = piece_of(origin, piece)
        return pltpu.make_async_remote_copy(
            src_ref=part_of,
            dst_ref=part_of,
            send_sem=z_send.at[way, t, piece],
            recv_sem=z_recv.at[way, t, piece],
            device_id=(ahead, y, z),
            device_id_type=MESH,
        )

    def has_ahead(way):
        return x < nx - 1 if way == 0 else x > 0

    def has_origin(way, t):
        return x >= t if way == 0 else x <= nx - 1 - t

    for step in range(RIGHT_STEPS):
        for copy in right_copies[step]:
            copy.wait_recv()
        gather_sums(right_in, right_all.at[x], step, RIGHT_STEPS)
        for piece in range(step * PARTS, (step + 1) * PARTS):
            for way in range(2):

                @pl.when(has_ahead(way))
                def _():
                    pass_on(way, 0, piece).start()

    for copy in left_copies:
        copy.wait_recv()
    gather_sums(left_in, left_all, 0, 1)

    left_copy = pltpu.make_async_remote_copy(
        src_ref=left_all,
        dst_ref=left_far,
        send_sem=far_sems.at[0],
        recv_sem=far_sems.at[1],
        device_id=(helper, y, z),
        device_id_type=MESH,
    )

    @pl.when(is_end)
    def _():
        left_copy.start()
        right_all[nx - 1 - end] = jnp.zeros(right_all.shape[1:], right_all.dtype)

    for t in range(1, nx - 1):
        for piece in range(pieces):
            for way in range(2):

                @pl.when(has_origin(way, t))
                def _():
                    pltpu.make_async_remote_copy(
                        src_ref=piece_of(x, piece),
                        dst_ref=piece_of(x - t if way == 0 else x + t, piece),
                        send_sem=z_send.at[way, t - 1, piece],
                        recv_sem=z_recv.at[way, t - 1, piece],
                        device_id=(x, y, z),
                        device_id_type=MESH,
                    ).wait_recv()
                    if t < nx - 2:

                        @pl.when(has_ahead(way))
                        def _():
                            pass_on(way, t, piece).start()

    def multiply(left, target, send):
        for c in range(block):
            triangle = lax.dot_general(
                left[c],
                right_all[:, c].reshape(nx * rows, LANES),
                (((1,), (1,)), ((), ())),
                preferred_element_type=jnp.float32,
            )
            spread[pl.ds(c, rows, stride=block), :] = triangle
        for q in range(tiles):
            swapped = swap_groups(
                [spread[pl.ds((q * per_tile + a) * block, block), :] for a in range(per_tile)], width
            )
            for d in range(plane):
                target[d, q] = swapped[d].astype(jnp.bfloat16)
            if (q + 1) % per_step == 0:
                send(q // per_step)

    def far_copy(index, step):
        d = (nx - 1 - end) * owners + index
        return pltpu.make_async_remote_copy(
            src_ref=tri_far.at[d, pl.ds(step * per_step, per_step)],
            dst_ref=tri_in.at[me, pl.ds(step * per_step, per_step)],
            send_sem=far_send.at[step, index],
            recv_sem=tri_sems.at[1, step, lax.rem(d - me + plane, plane)],
            device_id=(end, d // nz, lax.rem(d, nz)),
            device_id_type=MESH,
        )

    def tri_copy(t, step):
        d, device = peer(t)
        return pltpu.make_async_remote_copy(
            src_ref=tri_out.at[d, pl.ds(step * per_step, per_step)],
            dst_ref=tri_in.at[me, pl.ds(step * per_step, per_step)],
            send_sem=tri_sems.at[0, step, t],
            recv_sem=tri_sems.at[1, step, t],
            device_id=device,
            device_id_type=MESH,
        )

    def send_far(step):
        for index in range(owners):
            far_copy(index, step).start()

    def send(step):
        for t in range(1, plane):

            @pl.when(jnp.logical_not(is_left_out(peer(t)[0])))
            def _():
                tri_copy(t, step).start()

    def receive(step):
        @pl.when(is_left_out(me))
        def _():
            tri_copy(0, step).wait_recv()

        for t in range(1, plane):
            tri_copy(t, step).wait_recv()

    @pl.when(is_helper)
    def _():
        left_copy.wait_recv()
        multiply(left_far, tri_far, send_far)

    multiply(left_all, tri_out, send)

    @pl.when(jnp.logical_not(is_left_out(me)))
    def _():
        tri_in[me] = tri_out[me]

    for load in loads[6:]:
        load.wait()
    for q in range(tiles):
        if q % per_step == 0:
            receive(q // per_step)
        lanes = slice(q * LANES, (q + 1) * LANES)
        sums = tri_in[:, q].reshape(hidden, LANES).astype(jnp.float32)
        centered = sums - jnp.mean(sums, axis=0, keepdims=True)
        variance = jnp.mean(centered * centered, axis=0, keepdims=True)
        scaled = (centered * lax.rsqrt(variance + EPSILON)).T
        tri_normed = (scaled * out_gain_ref[...] + out_bias_ref[...]).astype(jnp.bfloat16)
        mixed = jnp.dot(tri_normed, out_weight_ref[...], preferred_element_type=jnp.float32)
        out_ref[q * per_tile : (q + 1) * per_tile] = (
            (gating_ref[lanes, :] * mixed).astype(jnp.bfloat16).reshape(per_tile, width, channels)
        )

    for copy in sum(right_copies, left_copies):
        copy.wait_send()
    for t in range(1, plane):

        @pl.when(jnp.logical_not(is_left_out(peer(t)[0])))
        def _():
            for step in range(TRI_STEPS):
                tri_copy(t, step).wait_send()

    @pl.when(is_helper)
    def _():
        for index in range(owners):
            for step in range(TRI_STEPS):
                far_copy(index, step).wait_send()

    @pl.when(is_end)
    def _():
        left_copy.wait_send()

    for t in range(nx - 2):
        for piece in range(pieces):
            for way in range(2):

                @pl.when(jnp.logical_and(has_ahead(way), has_origin(way, t)))
                def _():
                    pass_on(way, t, piece).wait_send()


def fused(nx, ny, nz, *arguments):
    pair, pair_mask, in_gain, in_bias, proj_weight, gate_weight, out_gain, out_bias, out_weight = arguments
    rows, width, channels = pair.shape
    hidden = proj_weight.shape[1] // 4
    plane = ny * nz
    block = hidden // plane
    tiles = rows * width // LANES
    travelling = pltpu.VMEM((plane, tiles, block, LANES), jnp.bfloat16)
    return pl.pallas_call(
        functools.partial(kernel, nx, ny, nz),
        out_shape=jax.ShapeDtypeStruct(pair.shape, jnp.bfloat16),
        in_specs=[pl.BlockSpec(memory_space=pltpu.HBM)] * 9,
        out_specs=pl.BlockSpec(memory_space=pltpu.VMEM),
        scratch_shapes=[travelling] * 6
        + [
            pltpu.VMEM((nx, block, rows, LANES), jnp.bfloat16),
            pltpu.VMEM((block, rows, LANES), jnp.bfloat16),
            pltpu.VMEM((block, rows, LANES), jnp.bfloat16),
            travelling,
            pltpu.VMEM((block * rows, LANES), jnp.float32),
            pltpu.VMEM((rows * width, channels), jnp.bfloat16),
            pltpu.VMEM((rows * width, channels), jnp.float32),
        ]
        + [pltpu.SemaphoreType.DMA((2, steps, plane)) for steps in (RIGHT_STEPS, 1, TRI_STEPS)]
        + [pltpu.SemaphoreType.DMA((2, nx - 2, RIGHT_STEPS * PARTS))] * 2
        + [pltpu.SemaphoreType.DMA((2,)), pltpu.SemaphoreType.DMA((TRI_STEPS, rows // width))]
        + [
            pltpu.VMEM(pair.shape, pair.dtype),
            pltpu.VMEM((width, rows), pair_mask.dtype),
            pltpu.VMEM((1, in_gain.size), in_gain.dtype),
            pltpu.VMEM((1, in_bias.size), in_bias.dtype),
            pltpu.VMEM(proj_weight.shape, proj_weight.dtype),
            pltpu.VMEM(gate_weight.shape, gate_weight.dtype),
            pltpu.VMEM((1, out_gain.size), out_gain.dtype),
            pltpu.VMEM((1, out_bias.size), out_bias.dtype),
            pltpu.VMEM(out_weight.shape, out_weight.dtype),
            pltpu.SemaphoreType.DMA((9,)),
        ],
        compiler_params=pltpu.CompilerParams(collective_id=0, has_side_effects=True),
    )(
        pair,
        pair_mask.T,
        in_gain.reshape(1, -1),
        in_bias.reshape(1, -1),
        proj_weight,
        gate_weight,
        out_gain.reshape(1, -1),
        out_bias.reshape(1, -1),
        out_weight,
    )


def solution(mesh):
    nx, ny, nz = mesh.shape["gx"], mesh.shape["gy"], mesh.shape["gz"]
    plane = ny * nz

    def on_device(pair, *others):
        rows, width, channels = pair.shape
        hidden = others[3].shape[1] // 4
        fits = (
            width * plane == LANES
            and rows * nx == LANES
            and rows % plane == 0
            and rows % width == 0
            and rows * width % (RIGHT_STEPS * TRI_STEPS * LANES) == 0
            and nx >= 4
            and channels % LANES == 0
            and hidden % (16 * plane) == 0
        )
        if fits:
            return fused(nx, ny, nz, pair, *others)
        return with_collectives(pair, *others)

    return jax.shard_map(
        on_device,
        mesh=mesh,
        in_specs=(
            P("gx", ("gy", "gz"), None),
            P("gx", ("gy", "gz")),
            P(),
            P(),
            P(),
            P(),
            P(),
            P(),
            P(),
        ),
        out_specs=P("gx", ("gy", "gz"), None),
        check_vma=False,
    )
```
